128 devices in a mesh: cell: 8 (over z_hi, y), idx: 16 (over z_lo, x, core).
Axes of the slice: x: 4, y: 4, z: 4 (z_hi: 2, z_lo: 2; z = z_hi * 2 + z_lo), core: 2. Of those that a mesh axis runs over, the one named last changes fastest.
Arguments:
- coeffs: bfloat16 [12288, 2048], P('cell', 'idx'), may hold values from -6 to 6
- tensor: bfloat16 [16, 2048, 2048], P('cell', 'idx'), may hold values from -0.0029296875 to 0.0029296875
Outputs:
- collision: float32 [16, 12288], P(None, ('cell', 'idx'))
The draws below stay inside these ranges and needn't reach their ends.
All inputs are finite; a program needn't handle non-finite values.
Results may differ from the reference program's by a relative error of at most 0.0003.
Values may be sent and summed in bfloat16 or wider, within the bound.
A program may use at most 64 MiB of HBM per device.

```python
import jax
import jax.numpy as jnp
from jax import lax

K = 2048
KO = 16
CELLS = 12288


def levels(rng, shape, shards, low, largest):
    def one(axis_at, blocks):
        heights = jax.random.uniform(jax.random.fold_in(jax.random.fold_in(rng, 6), axis_at), (blocks,), jnp.float32, low / len(shards), largest / len(shards))
        return jnp.repeat(jnp.exp(heights), shape[axis_at] // blocks).reshape((-1,) + (1,) * (len(shape) - axis_at - 1))

    level = one(*shards[0])
    for cut in shards[1:]:
        level = level * one(*cut)
    return level


def scatter_about(stream_key, extent, spread, limit, split=(), held_as=jnp.bfloat16):
    result = jax.random.normal(stream_key, extent, jnp.float32) * spread
    if len(split) > 0:
        result = levels(stream_key, extent, split, -0.22, 0.18) * result
    return jnp.clip(result, min=-limit, max=limit).astype(held_as)


def setup_inputs(seed: int = 0) -> dict:
    streams_of = jax.random.split(jax.random.key(seed), 3)
    return {
        "coeffs": scatter_about(streams_of[0], (CELLS, K), 1.0, 6.0, ((0, 8), (1, 16))),
        "tensor": scatter_about(streams_of[1], (KO, K, K), (K * K) ** -0.5, 0.0029296875, ((0, 8), (1, 16))),
    }


def reference(coeffs, tensor):
    values = coeffs.astype(jnp.float32)

    def one_output(slab):
        mixed = jnp.dot(coeffs, jnp.transpose(slab), preferred_element_type=jnp.float32)
        return jnp.sum(mixed * values, axis=1)

    return lax.map(one_output, tensor)
```

```python
import jax
import jax.numpy as jnp
from jax import lax
from jax.experimental import pallas as pl
from jax.experimental.pallas import tpu as pltpu
from jax.sharding import PartitionSpec as P

F32 = jnp.float32
BF16 = jnp.bfloat16
NX = 4
NY = 4
ROW_OF_DY = {0: 0, 1: 1, 3: 2, 2: 3}
PIECES = (0, 1, 3, 2)
ONWARD_UP = (0, 3)
ONWARD_DOWN = (1, 2)


def flip(bit, other):
    return 1 - bit if other else bit


def kernel(
    x_hbm, t_hbm, o_ref,
    xin, outbox, slab, xi, xj, outp, stage, arrived,
    in_sem, t_sem, y_send, z_send, x_send, pair_send, out_send,
    slab_recv, xi_recv, xj_recv, out_recv,
):
    cell = lax.axis_index("cell")
    idx = lax.axis_index("idx")
    zh = cell // NY
    y = cell % NY
    core = idx % 2
    x = (idx // 2) % NX
    zl = idx // (2 * NX)
    cells, width = x_hbm.shape
    owners = lax.axis_size("idx")
    own = cells // owners

    def device(dx=0, dy=0, e=0, other_core=0):
        return {
            "cell": flip(zh, e // 2) * NY + (y + dy) % NY,
            "idx": (flip(zl, e % 2) * NX + (x + dx) % NX) * 2 + flip(core, other_core),
        }

    def copy_to(src, dst, send, recv, dev):
        return pltpu.make_async_remote_copy(
            src_ref=src, dst_ref=dst, send_sem=send, recv_sem=recv,
            device_id=dev, device_id_type=pl.DeviceIdType.MESH,
        )

    x_in = pltpu.make_async_copy(x_hbm, xin, in_sem)
    x_in.start()

    def part_of(e):
        return slab.at[0] if e == 0 else outbox.at[e - 1]

    for e in PIECES:
        for dx in range(NX):
            block = (flip(zl, e % 2) * NX + (x + dx) % NX) * 2 + flip(zh, e // 2)
            pltpu.make_async_copy(
                t_hbm.at[:, pl.ds(pl.multiple_of(block * width, width), width)],
                part_of(e).at[:, pl.ds(dx * width, width)],
                t_sem.at[e],
            ).start()

    barrier = pltpu.get_barrier_semaphore()
    peers = [
        device(dx=dx, e=e, other_core=oc)
        for e in range(4) for dx in range(NX) for oc in range(2)
        if (e, dx, oc) != (0, 0, 0)
    ] + [device(dy=1), device(dy=3)]
    for peer in peers:
        pl.semaphore_signal(
            barrier, inc=1, device_id=peer, device_id_type=pl.DeviceIdType.MESH
        )

    x_in.wait()
    for t in range(cells // width):
        xi[0, :, t * width : (t + 1) * width] = jnp.transpose(
            xin[t * width : (t + 1) * width, :]
        )

    source = core == zh

    @pl.when(source)
    def _():
        xj[0, :width, :] = xi[0]

    for e in PIECES:
        pltpu.make_async_copy(part_of(e), part_of(e), t_sem.at[e]).wait()

    pl.semaphore_wait(barrier, len(peers))

    def y_copy(dy, e, up):
        n = (0 if up else 6) + (PIECES.index(e) if dy == 0 else 4 + (ONWARD_UP if up else ONWARD_DOWN).index(e))
        there = (dy - (1 if up else -1)) % NY
        return copy_to(
            slab.at[dy * 4 + e], slab.at[there * 4 + e],
            y_send.at[n], slab_recv.at[there * 4 + e], device(dy=1 if up else 3),
        )

    def z_copy_t(e):
        return copy_to(
            outbox.at[e - 1], slab.at[e], z_send.at[e - 1], slab_recv.at[e], device(e=e)
        )

    def z_copy_x(e):
        return copy_to(xi.at[0], xi.at[e], z_send.at[2 + e], xi_recv.at[e], device(e=e))

    def block_of(hr, dx):
        return xj.at[hr, pl.ds(dx * width, width)]

    def x_copy(hr, dx):
        return copy_to(
            xi.at[2 * hr], block_of(hr, NX - dx),
            x_send.at[hr * 3 + dx - 1], xj_recv.at[hr * 4 + NX - dx], device(dx=dx),
        )

    def pair_copy(hr, dx):
        src = xi.at[2 * hr] if dx == 0 else block_of(hr, dx)
        return copy_to(
            src, block_of(hr, dx),
            pair_send.at[hr * 4 + dx], xj_recv.at[hr * 4 + dx], device(other_core=1),
        )

    def got_slab(dy, e):
        there = slab.at[dy * 4 + e]
        pltpu.make_async_copy(there, there, slab_recv.at[dy * 4 + e]).wait()

    def got_xi(e):
        pltpu.make_async_copy(xi.at[e], xi.at[e], xi_recv.at[e]).wait()

    def got_xj(hr, dx):
        there = block_of(hr, dx)
        pltpu.make_async_copy(there, there, xj_recv.at[hr * 4 + dx]).wait()

    def y_own(e):
        y_copy(0, e, True).start()
        y_copy(0, e, False).start()

    def take_xj(hr, dxs):
        @pl.when(source)
        def _():
            for dx in dxs:
                got_xj(hr, dx)
                pair_copy(hr, dx).start()

    def have_xj(hr):
        @pl.when(jnp.logical_not(source))
        def _():
            for dx in range(NX):
                got_xj(hr, dx)

    def unit(dy, eh, hr):
        row = ROW_OF_DY[dy] * 4 + eh * 2

        def tile(n, _):
            cols = pl.ds(pl.multiple_of(n * 256, 256), 256)
            w = xj[hr, :, cols]
            total = None
            for el in range(2):
                mixed = jnp.dot(slab[dy * 4 + eh * 2 + el], w, preferred_element_type=F32)
                rows = xi[hr * 2 + el, :, cols].astype(F32)
                terms = mixed.reshape(2, width, 256) * rows[None]
                part = jnp.sum(terms.reshape(2, width // 8, 8, 256), axis=1)
                total = part if total is None else total + part
            outp[hr, row : row + 2, cols] = jnp.sum(total, axis=1)
            return 0

        lax.fori_loop(0, cells // 256, tile, 0)

    def send_out(b):
        for hr in range(2):
            rows = outp[hr, b * 8 : b * 8 + 8, :]
            for q in range(owners):
                first = q * own // 128 * 128
                shift = q * own - first
                window = rows[:, first : first + 256] if first + 256 <= cells else rows[:, first : first + 128]
                if shift:
                    window = pltpu.roll(window, window.shape[1] - shift, 1)
                stage[b, hr * owners + q] = window[:, :128]

        def send(j, _):
            hr = j // owners
            q = (idx + j) % owners
            copy_to(
                stage.at[b, hr * owners + q], arrived.at[b, hr * owners + idx],
                out_send.at[b], out_recv.at[b],
                {"cell": (zh + hr - 2 * zh * hr) * NY + y, "idx": q},
            ).start()
            return 0

        lax.fori_loop(1, 2 * owners, send, 0)
        arrived[b, idx] = stage[b, idx]

    def all_but_one(ref, b):
        return ref.at[b, pl.ds(0, 2 * owners - 1)]

    y_own(0)

    @pl.when(source)
    def _():
        for e in (1, 3, 2):
            z_copy_t(e).start()
        for dx in (1, 3, 2):
            x_copy(0, dx).start()
        pair_copy(0, 0).start()
        for e in (1, 3, 2):
            z_copy_x(e).start()

    @pl.when(jnp.logical_not(source))
    def _():
        z_copy_x(2).start()
        for e in (1, 3, 2):
            z_copy_t(e).start()
        for e in (1, 3):
            z_copy_x(e).start()

    got_slab(0, 1)
    y_own(1)
    got_slab(0, 3)
    y_own(3)
    take_xj(0, (1, 3))
    got_slab(3, 0)
    y_copy(3, 0, True).start()
    got_xi(2)

    @pl.when(source)
    def _():
        for dx in (1, 3, 2):
            x_copy(1, dx).start()
        pair_copy(1, 0).start()
        xj[1, :width, :] = xi[2]

    got_slab(0, 2)
    y_own(2)
    take_xj(0, (2,))
    got_slab(1, 1)
    y_copy(1, 1, False).start()
    got_xi(1)
    have_xj(0)
    unit(0, 0, 0)
    unit(0, 1, 0)
    got_slab(3, 1)
    got_slab(1, 0)
    unit(1, 0, 0)
    take_xj(1, (1, 3))
    unit(3, 0, 0)
    got_slab(3, 3)
    y_copy(3, 3, True).start()
    take_xj(1, (2,))
    got_xi(3)
    have_xj(1)
    unit(0, 0, 1)
    unit(0, 1, 1)
    got_slab(1, 2)
    y_copy(1, 2, False).start()
    unit(1, 0, 1)
    unit(3, 0, 1)
    got_slab(1, 3)
    unit(1, 1, 0)
    unit(1, 1, 1)
    send_out(0)
    got_slab(3, 2)
    unit(3, 1, 0)
    unit(3, 1, 1)
    got_slab(2, 0)
    got_slab(2, 1)
    unit(2, 0, 0)
    unit(2, 0, 1)
    got_slab(2, 3)
    got_slab(2, 2)
    unit(2, 1, 0)
    unit(2, 1, 1)
    send_out(1)

    for b in range(2):
        pltpu.make_async_copy(all_but_one(arrived, b), all_but_one(arrived, b), out_recv.at[b]).wait()
        same = jnp.sum(arrived[b, :owners], axis=0)
        crossed = jnp.sum(arrived[b, owners:], axis=0)
        for r in range(4):
            dy = [d for d, place in ROW_OF_DY.items() if place == b * 2 + r // 2][0]
            eh = r % 2
            k = (flip(zh, eh) * NY + (y + dy) % NY) * 2
            for kk in range(2):
                a = r * 2 + kk
                c = (r ^ 1) * 2 + kk
                o_ref[pl.ds(k + kk, 1), :] = (same[a : a + 1] + crossed[c : c + 1])[:, :own]

    for e in PIECES:
        y_copy(0, e, True).wait_send()
        y_copy(0, e, False).wait_send()
    for e in ONWARD_UP:
        y_copy(3, e, True).wait_send()
    for e in ONWARD_DOWN:
        y_copy(1, e, False).wait_send()
    for e in (1, 2, 3):
        z_copy_t(e).wait_send()
        z_copy_x(e).wait_send()

    @pl.when(source)
    def _():
        for hr in range(2):
            for dx in range(NX):
                pair_copy(hr, dx).wait_send()
                if dx:
                    x_copy(hr, dx).wait_send()

    for b in range(2):
        pltpu.make_async_copy(all_but_one(stage, b), all_but_one(stage, b), out_send.at[b]).wait()


def shards(coeffs, tensor):
    cells, width = coeffs.shape
    outputs, inner, full = tensor.shape
    owners = lax.axis_size("idx")
    rows = outputs * inner
    return pl.pallas_call(
        kernel,
        out_shape=jax.ShapeDtypeStruct((16, cells // owners), F32),
        in_specs=[pl.BlockSpec(memory_space=pl.ANY)] * 2,
        out_specs=pl.BlockSpec(memory_space=pltpu.VMEM),
        scratch_shapes=[
            pltpu.VMEM((cells, width), BF16),
            pltpu.VMEM((3, rows, NX * width), BF16),
            pltpu.VMEM((16, rows, NX * width), BF16),
            pltpu.VMEM((4, width, cells), BF16),
            pltpu.VMEM((2, NX * width, cells), BF16),
            pltpu.VMEM((2, 16, cells), F32),
            pltpu.VMEM((2, 2 * owners, 8, 128), F32),
            pltpu.VMEM((2, 2 * owners, 8, 128), F32),
            pltpu.SemaphoreType.DMA,
            pltpu.SemaphoreType.DMA((4,)),
            pltpu.SemaphoreType.DMA((12,)),
            pltpu.SemaphoreType.DMA((6,)),
            pltpu.SemaphoreType.DMA((6,)),
            pltpu.SemaphoreType.DMA((8,)),
            pltpu.SemaphoreType.DMA((2,)),
            pltpu.SemaphoreType.DMA((16,)),
            pltpu.SemaphoreType.DMA((4,)),
            pltpu.SemaphoreType.DMA((8,)),
            pltpu.SemaphoreType.DMA((2,)),
        ],
        compiler_params=pltpu.CompilerParams(
            collective_id=0, has_side_effects=True, vmem_limit_bytes=48 * 1024 * 1024
        ),
    )(coeffs, tensor.reshape(rows, full))


def solution(mesh):
    return jax.shard_map(
        shards,
        mesh=mesh,
        in_specs=(P("cell", "idx"), P("cell", "idx", None)),
        out_specs=P(None, ("cell", "idx")),
        check_vma=False,
    )
```

```python
import jax
import jax.numpy as jnp
from jax import lax
from jax.experimental import pallas as pl
from jax.experimental.pallas import tpu as pltpu
from jax.sharding import PartitionSpec as P

F32 = jnp.float32
BF16 = jnp.bfloat16
NX = 4
NY = 4
ROW_OF_DY = {0: 0, 1: 1, 3: 2, 2: 3}


def flip(bit, other):
    return 1 - bit if other else bit


def kernel(
    x_hbm, t_hbm, o_ref,
    xin, outbox, passing, slab, xi, xj, outp, stage, arrived,
    in_sem, t_sem, y_send, z_send, x_send, pair_send, out_send,
    slab_recv, pass_recv, xi_recv, xj_recv, out_recv, ready, pair_ready,
):
    cell = lax.axis_index("cell")
    idx = lax.axis_index("idx")
    zh = cell // NY
    y = cell % NY
    core = idx % 2
    x = (idx // 2) % NX
    zl = idx // (2 * NX)
    cells, width = x_hbm.shape
    line = NX * width
    owners = lax.axis_size("idx")
    own = cells // owners

    def device(dx=0, dy=0, e=0, other_core=0):
        return {
            "cell": flip(zh, e // 2) * NY + (y + dy) % NY,
            "idx": (flip(zl, e % 2) * NX + (x + dx) % NX) * 2 + flip(core, other_core),
        }

    def copy_to(src, dst, send, recv, dev):
        return pltpu.make_async_remote_copy(
            src_ref=src, dst_ref=dst, send_sem=send, recv_sem=recv,
            device_id=dev, device_id_type=pl.DeviceIdType.MESH,
        )

    def signal(sem, dev):
        pl.semaphore_signal(sem, inc=1, device_id=dev, device_id_type=pl.DeviceIdType.MESH)

    barrier = pltpu.get_barrier_semaphore()
    peers = [device(dy=1), device(dy=3), device(other_core=1)]
    peers += [device(dx=dx) for dx in (1, 2, 3)] + [device(e=e) for e in (1, 2, 3)]
    for peer in peers:
        signal(barrier, peer)

    x_in = pltpu.make_async_copy(x_hbm, xin, in_sem)
    x_in.start()

    def part_of(eh, kk):
        return outbox.at[kk] if eh else slab.at[kk]

    for eh in range(2):
        for kk in range(2):
            for el in range(2):
                for dx in range(NX):
                    block = (flip(zl, el) * NX + (x + dx) % NX) * 2 + flip(zh, eh)
                    pltpu.make_async_copy(
                        t_hbm.at[pl.ds(kk * width, width), pl.ds(pl.multiple_of(block * width, width), width)],
                        part_of(eh, kk).at[:, pl.ds(el * line + dx * width, width)],
                        t_sem.at[eh * 2 + kk],
                    ).start()

    x_in.wait()
    for t in range(cells // width):
        xi[0, :, t * width : (t + 1) * width] = jnp.transpose(
            xin[t * width : (t + 1) * width, :]
        )

    source = core == zh

    def on_source(f):
        pl.when(source)(f)

    def on_other(f):
        pl.when(jnp.logical_not(source))(f)

    @on_source
    def _():
        xj[0, :width, :] = xi[0]

    for eh in range(2):
        for kk in range(2):
            pltpu.make_async_copy(part_of(eh, kk), part_of(eh, kk), t_sem.at[eh * 2 + kk]).wait()

    pl.semaphore_wait(barrier, len(peers))

    for dx in (1, 2, 3):
        signal(ready, device(dx=dx))

    def slot(dy, eh, kk):
        return dy * 4 + eh * 2 + kk

    def y_copy(dy, eh, kk, up):
        n = (0 if up else 6) + (eh * 2 + kk if dy == 0 else 4 + eh)
        there = slot((dy - (1 if up else -1)) % NY, eh, kk)
        return copy_to(
            slab.at[slot(dy, eh, kk)], slab.at[there],
            y_send.at[n], slab_recv.at[there], device(dy=1 if up else 3),
        )

    def block_of(hr, el, dx):
        return xj.at[hr, pl.ds(el * line + dx * width, width)]

    def half_of(hr, el, part):
        return xj.at[hr, pl.ds(el * line + 2 * width + part * (width // 2), width // 2)]

    def number(hr, el, dx):
        return (hr * 2 + el) * NX + dx

    def z_copy_t(kk):
        return copy_to(outbox.at[kk], passing.at[kk], z_send.at[kk], pass_recv.at[kk], device(e=3 if kk else 1))

    def z_onward_t(kk):
        there = slot(0, 1, kk)
        return copy_to(
            passing.at[kk], slab.at[there], z_send.at[2 + kk], slab_recv.at[there], device(e=1 if kk else 3)
        )

    def z_onward_x(hr):
        return copy_to(block_of(hr, 1, 0), xi.at[1], z_send.at[5 + hr], xi_recv, device(e=1 if hr else 3))

    def z_copy_j(e):
        hr = e // 2
        return copy_to(
            xi.at[0], block_of(hr, 1, 0), z_send.at[4], xj_recv.at[number(hr, 1, 0)], device(e=e)
        )

    def first_of(hr, el):
        return block_of(hr, el, 0) if el else xi.at[hr]

    def x_copy(hr, el, dx):
        n = number(hr, el, 0 if dx == 1 else 1)
        there = NX - dx
        return copy_to(
            first_of(hr, el), block_of(hr, el, there),
            x_send.at[n], xj_recv.at[number(hr, el, there)], device(dx=dx),
        )

    def x_onward(hr, el, dx):
        part = 0 if dx == 1 else 1
        src = xj.at[hr, pl.ds(el * line + dx * width + part * (width // 2), width // 2)]
        return copy_to(
            src, half_of(hr, el, part), x_send.at[number(hr, el, 2 + part)],
            xj_recv.at[number(hr, el, 2)], device(dx=NX - dx),
        )

    def pair_copy(hr, el, dx):
        src = first_of(hr, el) if dx == 0 else block_of(hr, el, dx)
        n = number(hr, el, dx)
        return copy_to(
            src, block_of(hr, el, dx), pair_send.at[n], xj_recv.at[n], device(other_core=1)
        )

    def got_slab(dy, eh, kk):
        there = slab.at[slot(dy, eh, kk)]
        pltpu.make_async_copy(there, there, slab_recv.at[slot(dy, eh, kk)]).wait()

    def got_passing(kk):
        pltpu.make_async_copy(passing.at[kk], passing.at[kk], pass_recv.at[kk]).wait()

    def got_xi():
        pltpu.make_async_copy(xi.at[1], xi.at[1], xi_recv).wait()

    def got_xj(hr, el, dx):
        there = block_of(hr, el, dx)
        pltpu.make_async_copy(there, there, xj_recv.at[number(hr, el, dx)]).wait()

    def y_own(eh, kk):
        y_copy(0, eh, kk, True).start()
        y_copy(0, eh, 1 - kk, False).start()

    def y_onward(eh):
        y_copy(3, eh, 0, True).start()
        y_copy(1, eh, 1, False).start()

    def spread(hr, el):
        x_copy(hr, el, 1).start()
        x_copy(hr, el, 3).start()
        pair_copy(hr, el, 0).start()

    def start_group(hr, el):
        @on_source
        def _():
            if el:
                got_xj(hr, el, 0)
            elif hr:
                got_xi()
            spread(hr, el)
            if hr and not el:
                xj[1, :width, :] = xi[1]

    def pass_on(hr, el):
        @on_source
        def _():
            for dx in (1, 3):
                got_xj(hr, el, dx)
                x_onward(hr, el, dx).start()
                pair_copy(hr, el, dx).start()

    def end_group(hr, el):
        @on_source
        def _():
            got_xj(hr, el, 2)
            pair_copy(hr, el, 2).start()

    def have_group(hr, el):
        @on_other
        def _():
            for dx in range(NX):
                got_xj(hr, el, dx)

    begun = set()

    def unit(pieces, hr, els):
        deep = pl.ds(els[0] * line, len(els) * line)

        def tile(n, _):
            cols = pl.ds(pl.multiple_of(n * 256, 256), 256)
            w = xj[hr, deep, cols]
            rows = xi[hr, :, cols].astype(F32)
            for dy, eh in pieces:
                at = slot(dy, eh, 0)
                left = slab[at : at + 2, :, deep].reshape(2 * width, len(els) * line)
                mixed = jnp.dot(left, w, preferred_element_type=F32)
                terms = mixed.reshape(2, width, 256) * rows[None]
                part = jnp.sum(terms.reshape(2, width // 8, 8, 256), axis=1)
                out = jnp.sum(part, axis=1)
                row = ROW_OF_DY[dy] * 4 + eh * 2
                if (dy, eh, hr) in begun:
                    out = out + outp[hr, row : row + 2, cols]
                outp[hr, row : row + 2, cols] = out
            return 0

        lax.fori_loop(0, cells // 256, tile, 0, unroll=True)
        begun.update((dy, eh, hr) for dy, eh in pieces)

    def send_out(b):
        for hr in range(2):
            rows = outp[hr, b * 8 : b * 8 + 8, :]
            for q in range(owners):
                first = q * own // 128 * 128
                shift = q * own - first
                window = rows[:, first : first + 256] if first + 256 <= cells else rows[:, first : first + 128]
                if shift:
                    window = pltpu.roll(window, window.shape[1] - shift, 1)
                stage[b, hr * owners + q] = window[:, :128]

        def send(j, _):
            hr = j // owners
            q = (idx + j) % owners
            copy_to(
                stage.at[b, hr * owners + q], arrived.at[b, hr * owners + idx],
                out_send.at[b], out_recv.at[b],
                {"cell": (zh + hr - 2 * zh * hr) * NY + y, "idx": q},
            ).start()
            return 0

        lax.fori_loop(1, 2 * owners, send, 0)
        arrived[b, idx] = stage[b, idx]

    def all_but_one(ref, b):
        return ref.at[b, pl.ds(0, 2 * owners - 1)]

    y_own(0, 0)
    y_own(0, 1)

    @on_source
    def _():
        z_copy_j(1).start()
        spread(0, 0)

    @on_other
    def _():
        z_copy_j(3).start()

    z_copy_t(0).start()
    z_copy_t(1).start()

    pass_on(0, 0)
    got_slab(3, 0, 0)
    got_slab(1, 0, 1)
    y_onward(0)
    start_group(0, 1)
    end_group(0, 0)
    start_group(1, 1)
    on_source(z_onward_x(1).start)
    for kk in range(2):
        got_passing(kk)
        z_onward_t(kk).start()
    on_source(z_onward_x(0).start)

    pass_on(0, 1)
    have_group(0, 0)
    got_slab(3, 0, 1)
    got_slab(1, 0, 0)
    unit(((0, 0), (1, 0), (3, 0)), 0, (0,))
    got_slab(0, 1, 0)
    y_copy(0, 1, 0, True).start()
    start_group(1, 0)
    end_group(0, 1)
    pass_on(1, 1)
    got_slab(0, 1, 1)
    y_copy(0, 1, 1, False).start()
    y_copy(0, 1, 1, True).start()
    y_copy(0, 1, 0, False).start()
    pl.semaphore_wait(ready, 3)
    signal(pair_ready, device(other_core=1))
    have_group(0, 1)
    unit(((0, 0), (1, 0), (3, 0)), 0, (1,))
    end_group(1, 1)
    got_slab(2, 0, 0)
    got_slab(2, 0, 1)
    unit(((2, 0), (0, 1)), 0, (0, 1))
    got_slab(3, 1, 0)
    got_slab(1, 1, 1)
    y_onward(1)
    pass_on(1, 0)
    on_other(got_xi)
    have_group(1, 1)
    unit(((0, 0), (0, 1), (1, 0), (3, 0), (2, 0)), 1, (1,))
    end_group(1, 0)
    got_slab(3, 1, 1)
    got_slab(1, 1, 0)
    unit(((1, 1), (3, 1)), 0, (0, 1))
    have_group(1, 0)
    unit(((0, 0), (0, 1), (1, 0), (3, 0), (2, 0)), 1, (0,))
    unit(((1, 1), (3, 1)), 1, (0, 1))
    pl.semaphore_wait(pair_ready, 1)
    send_out(0)
    got_slab(2, 1, 0)
    got_slab(2, 1, 1)
    unit(((2, 1),), 0, (0, 1))
    unit(((2, 1),), 1, (0, 1))
    send_out(1)

    for b in range(2):
        pltpu.make_async_copy(all_but_one(arrived, b), all_but_one(arrived, b), out_recv.at[b]).wait()
        same = jnp.sum(arrived[b, :owners], axis=0)
        crossed = jnp.sum(arrived[b, owners:], axis=0)
        for r in range(4):
            dy = [d for d, place in ROW_OF_DY.items() if place == b * 2 + r // 2][0]
            eh = r % 2
            k = (flip(zh, eh) * NY + (y + dy) % NY) * 2
            for kk in range(2):
                a = r * 2 + kk
                c = (r ^ 1) * 2 + kk
                o_ref[pl.ds(k + kk, 1), :] = (same[a : a + 1] + crossed[c : c + 1])[:, :own]

    for kk in range(2):
        for eh in range(2):
            y_copy(0, eh, kk, True).wait_send()
            y_copy(0, eh, kk, False).wait_send()
        y_copy(3, kk, 0, True).wait_send()
        y_copy(1, kk, 1, False).wait_send()
        z_copy_t(kk).wait_send()
        z_onward_t(kk).wait_send()
    z_copy_j(1).wait_send()

    @on_source
    def _():
        for hr in range(2):
            z_onward_x(hr).wait_send()
            for el in range(2):
                for dx in (1, 3):
                    x_copy(hr, el, dx).wait_send()
                    x_onward(hr, el, dx).wait_send()
                for dx in range(NX):
                    pair_copy(hr, el, dx).wait_send()

    for b in range(2):
        pltpu.make_async_copy(all_but_one(stage, b), all_but_one(stage, b), out_send.at[b]).wait()


def shards(coeffs, tensor):
    cells, width = coeffs.shape
    outputs, inner, full = tensor.shape
    owners = lax.axis_size("idx")
    return pl.pallas_call(
        kernel,
        out_shape=jax.ShapeDtypeStruct((16, cells // owners), F32),
        in_specs=[pl.BlockSpec(memory_space=pltpu.HBM)] * 2,
        out_specs=pl.BlockSpec(memory_space=pltpu.VMEM),
        scratch_shapes=[
            pltpu.VMEM((cells, width), BF16),
            pltpu.VMEM((2, inner, 2 * NX * width), BF16),
            pltpu.VMEM((2, inner, 2 * NX * width), BF16),
            pltpu.VMEM((16, inner, 2 * NX * width), BF16),
            pltpu.VMEM((2, width, cells), BF16),
            pltpu.VMEM((2, 2 * NX * width, cells), BF16),
            pltpu.VMEM((2, 16, cells), F32),
            pltpu.VMEM((2, 2 * owners, 8, 128), F32),
            pltpu.VMEM((2, 2 * owners, 8, 128), F32),
            pltpu.SemaphoreType.DMA,
            pltpu.SemaphoreType.DMA((4,)),
            pltpu.SemaphoreType.DMA((12,)),
            pltpu.SemaphoreType.DMA((7,)),
            pltpu.SemaphoreType.DMA((16,)),
            pltpu.SemaphoreType.DMA((16,)),
            pltpu.SemaphoreType.DMA((2,)),
            pltpu.SemaphoreType.DMA((16,)),
            pltpu.SemaphoreType.DMA((2,)),
            pltpu.SemaphoreType.DMA,
            pltpu.SemaphoreType.DMA((16,)),
            pltpu.SemaphoreType.DMA((2,)),
            pltpu.SemaphoreType.REGULAR,
            pltpu.SemaphoreType.REGULAR,
        ],
        compiler_params=pltpu.CompilerParams(
            collective_id=0, has_side_effects=True, vmem_limit_bytes=66200 * 1000
        ),
    )(coeffs, tensor.reshape(outputs * inner, full))


def solution(mesh):
    return jax.shard_map(
        shards,
        mesh=mesh,
        in_specs=(P("cell", "idx"), P("cell", "idx", None)),
        out_specs=P(None, ("cell", "idx")),
        check_vma=False,
    )
```

```python
import jax
import jax.numpy as jnp
from jax import lax
from jax.experimental import pallas as pl
from jax.experimental.pallas import tpu as pltpu
from jax.sharding import PartitionSpec as P

F32 = jnp.float32
BF16 = jnp.bfloat16
NX = 4
NY = 4
ROW_OF_DY = {0: 0, 1: 1, 3: 2, 2: 3}


def flip(bit, other):
    return 1 - bit if other else bit


def kernel(
    x_hbm, t_hbm, o_ref,
    xin, outbox, passing, slab, xi, xj, outp, stage, arrived,
    in_sem, t_sem, y_send, z_send, x_send, pair_send, out_send,
    slab_recv, pass_recv, xi_recv, xj_recv, out_recv, ready, pair_ready,
):
    cell = lax.axis_index("cell")
    idx = lax.axis_index("idx")
    zh = cell // NY
    y = cell % NY
    core = idx % 2
    x = (idx // 2) % NX
    zl = idx // (2 * NX)
    cells, width = x_hbm.shape
    line = NX * width
    owners = lax.axis_size("idx")
    own = cells // owners

    def device(dx=0, dy=0, e=0, other_core=0):
        return {
            "cell": flip(zh, e // 2) * NY + (y + dy) % NY,
            "idx": (flip(zl, e % 2) * NX + (x + dx) % NX) * 2 + flip(core, other_core),
        }

    def copy_to(src, dst, send, recv, dev):
        return pltpu.make_async_remote_copy(
            src_ref=src, dst_ref=dst, send_sem=send, recv_sem=recv,
            device_id=dev, device_id_type=pl.DeviceIdType.MESH,
        )

    def signal(sem, dev):
        pl.semaphore_signal(sem, inc=1, device_id=dev, device_id_type=pl.DeviceIdType.MESH)

    barrier = pltpu.get_barrier_semaphore()
    peers = [device(dy=1), device(dy=3), device(other_core=1)]
    peers += [device(dx=dx) for dx in (1, 2, 3)] + [device(e=e) for e in (1, 2, 3)]
    for peer in peers:
        signal(barrier, peer)

    x_in = pltpu.make_async_copy(x_hbm, xin, in_sem)
    x_in.start()

    def part_of(eh, kk):
        return outbox.at[kk] if eh else slab.at[kk]

    for eh in range(2):
        for kk in range(2):
            for el in range(2):
                for dx in range(NX):
                    block = (flip(zl, el) * NX + (x + dx) % NX) * 2 + flip(zh, eh)
                    pltpu.make_async_copy(
                        t_hbm.at[pl.ds(kk * width, width), pl.ds(pl.multiple_of(block * width, width), width)],
                        part_of(eh, kk).at[:, pl.ds(el * line + dx * width, width)],
                        t_sem.at[eh * 2 + kk],
                    ).start()

    x_in.wait()
    for t in range(cells // width):
        xi[0, :, t * width : (t + 1) * width] = jnp.transpose(
            xin[t * width : (t + 1) * width, :]
        )

    source = core == zh

    def on_source(f):
        pl.when(source)(f)

    def on_other(f):
        pl.when(jnp.logical_not(source))(f)

    @on_source
    def _():
        xj[0, :width, :] = xi[0]

    for eh in range(2):
        for kk in range(2):
            pltpu.make_async_copy(part_of(eh, kk), part_of(eh, kk), t_sem.at[eh * 2 + kk]).wait()

    pl.semaphore_wait(barrier, len(peers))

    for dx in (1, 2, 3):
        signal(ready, device(dx=dx))

    def slot(dy, eh, kk):
        return dy * 4 + eh * 2 + kk

    def y_copy(dy, eh, kk, up):
        n = (0 if up else 6) + (eh * 2 + kk if dy == 0 else 4 + eh)
        there = slot((dy - (1 if up else -1)) % NY, eh, kk)
        return copy_to(
            slab.at[slot(dy, eh, kk)], slab.at[there],
            y_send.at[n], slab_recv.at[there], device(dy=1 if up else 3),
        )

    def block_of(hr, el, dx):
        return xj.at[hr, pl.ds(el * line + dx * width, width)]

    def half_of(hr, el, part):
        return xj.at[hr, pl.ds(el * line + 2 * width + part * (width // 2), width // 2)]

    def number(hr, el, dx):
        return (hr * 2 + el) * NX + dx

    def z_copy_t(kk):
        return copy_to(outbox.at[kk], passing.at[kk], z_send.at[kk], pass_recv.at[kk], device(e=3 if kk else 1))

    def z_onward_t(kk):
        there = slot(0, 1, kk)
        return copy_to(
            passing.at[kk], slab.at[there], z_send.at[2 + kk], slab_recv.at[there], device(e=1 if kk else 3)
        )

    def z_onward_x(hr):
        return copy_to(block_of(hr, 1, 0), xi.at[1], z_send.at[5 + hr], xi_recv, device(e=1 if hr else 3))

    def z_copy_j(e):
        hr = e // 2
        return copy_to(
            xi.at[0], block_of(hr, 1, 0), z_send.at[4], xj_recv.at[number(hr, 1, 0)], device(e=e)
        )

    def first_of(hr, el):
        return block_of(hr, el, 0) if el else xi.at[hr]

    def x_copy(hr, el, dx):
        n = number(hr, el, {1: 0, 3: 1, 2: 2}[dx])
        there = NX - dx
        return copy_to(
            first_of(hr, el), block_of(hr, el, there),
            x_send.at[n], xj_recv.at[number(hr, el, there)], device(dx=dx),
        )

    def x_onward(hr, el, dx):
        part = 0 if dx == 1 else 1
        src = xj.at[hr, pl.ds(el * line + dx * width + part * (width // 2), width // 2)]
        return copy_to(
            src, half_of(hr, el, part), x_send.at[number(hr, el, 2 + part)],
            xj_recv.at[number(hr, el, 2)], device(dx=NX - dx),
        )

    def pair_copy(hr, el, dx):
        src = first_of(hr, el) if dx == 0 else block_of(hr, el, dx)
        n = number(hr, el, dx)
        return copy_to(
            src, block_of(hr, el, dx), pair_send.at[n], xj_recv.at[n], device(other_core=1)
        )

    def got_slab(dy, eh, kk):
        there = slab.at[slot(dy, eh, kk)]
        pltpu.make_async_copy(there, there, slab_recv.at[slot(dy, eh, kk)]).wait()

    def got_passing(kk):
        pltpu.make_async_copy(passing.at[kk], passing.at[kk], pass_recv.at[kk]).wait()

    def got_xi():
        pltpu.make_async_copy(xi.at[1], xi.at[1], xi_recv).wait()

    def got_xj(hr, el, dx):
        there = block_of(hr, el, dx)
        pltpu.make_async_copy(there, there, xj_recv.at[number(hr, el, dx)]).wait()

    def y_own(eh, kk):
        y_copy(0, eh, kk, True).start()
        y_copy(0, eh, 1 - kk, False).start()

    def spread(hr, el):
        x_copy(hr, el, 1).start()
        x_copy(hr, el, 3).start()
        pair_copy(hr, el, 0).start()

    def start_group(hr, el):
        @on_source
        def _():
            if el:
                got_xj(hr, el, 0)
            elif hr:
                got_xi()
            spread(hr, el)
            if hr and not el:
                xj[1, :width, :] = xi[1]

    def pass_on(hr, el):
        @on_source
        def _():
            for dx in (1, 3):
                got_xj(hr, el, dx)
                x_onward(hr, el, dx).start()
                pair_copy(hr, el, dx).start()

    def end_group(hr, el):
        @on_source
        def _():
            got_xj(hr, el, 2)
            pair_copy(hr, el, 2).start()

    def have_group(hr, el):
        @on_other
        def _():
            for dx in range(NX):
                got_xj(hr, el, dx)

    begun = set()

    def unit(pieces, hr, els):
        deep = pl.ds(els[0] * line, len(els) * line)

        def tile(n, _):
            cols = pl.ds(pl.multiple_of(n * 256, 256), 256)
            w = xj[hr, deep, cols]
            rows = xi[hr, :, cols].astype(F32)
            for dy, eh in pieces:
                at = slot(dy, eh, 0)
                left = slab[at : at + 2, :, deep].reshape(2 * width, len(els) * line)
                mixed = jnp.dot(left, w, preferred_element_type=F32)
                terms = mixed.reshape(2, width, 256) * rows[None]
                part = jnp.sum(terms.reshape(2, width // 8, 8, 256), axis=1)
                out = jnp.sum(part, axis=1)
                row = ROW_OF_DY[dy] * 4 + eh * 2
                if (dy, eh, hr) in begun:
                    out = out + outp[hr, row : row + 2, cols]
                outp[hr, row : row + 2, cols] = out
            return 0

        lax.fori_loop(0, cells // 256, tile, 0, unroll=True)
        begun.update((dy, eh, hr) for dy, eh in pieces)

    def send_out(b, hrs=(1, 0)):
        for hr in hrs:
            rows = outp[hr, b * 8 : b * 8 + 8, :]
            for q in range(owners):
                first = q * own // 128 * 128
                shift = q * own - first
                window = rows[:, first : first + 256] if first + 256 <= cells else rows[:, first : first + 128]
                if shift:
                    window = pltpu.roll(window, window.shape[1] - shift, 1)
                stage[b, hr * owners + q] = window[:, :128]

            for j in range(1 - hr, owners):
                q = (idx + j) % owners
                copy_to(
                    stage.at[b, hr * owners + q], arrived.at[b, hr * owners + idx],
                    out_send.at[b], out_recv.at[b],
                    {"cell": flip(zh, hr) * NY + y, "idx": q},
                ).start()

        if 0 in hrs:
            arrived[b, idx] = stage[b, idx]

    def all_but_one(ref, b):
        return ref.at[b, pl.ds(0, 2 * owners - 1)]

    y_own(0, 0)
    y_own(0, 1)

    @on_source
    def _():
        z_copy_j(1).start()
        spread(0, 0)

    z_copy_t(0).start()
    z_copy_t(1).start()
    on_other(z_copy_j(3).start)

    pass_on(0, 0)
    got_slab(3, 0, 0)
    got_slab(1, 0, 1)
    y_copy(3, 0, 0, True).start()
    y_copy(1, 0, 1, False).start()
    start_group(0, 1)
    end_group(0, 0)
    start_group(1, 1)
    on_source(z_onward_x(1).start)
    for kk in range(2):
        got_passing(kk)
        z_onward_t(kk).start()
    on_source(z_onward_x(0).start)

    pass_on(0, 1)
    have_group(0, 0)
    got_slab(3, 0, 1)
    got_slab(1, 0, 0)
    unit(((0, 0), (1, 0), (3, 0)), 0, (0,))
    got_slab(0, 1, 0)
    y_copy(0, 1, 0, True).start()
    start_group(1, 0)
    pass_on(1, 1)
    got_slab(0, 1, 1)
    y_copy(0, 1, 1, False).start()
    y_copy(0, 1, 1, True).start()
    y_copy(0, 1, 0, False).start()
    end_group(0, 1)
    pl.semaphore_wait(ready, 3)
    signal(pair_ready, device(other_core=1))
    unit(((0, 1),), 0, (0,))
    have_group(0, 1)
    unit(((0, 0), (1, 0), (3, 0), (0, 1)), 0, (1,))
    got_slab(3, 1, 0)
    y_copy(3, 1, 0, True).start()
    pass_on(1, 0)
    got_slab(1, 1, 1)
    y_copy(1, 1, 1, False).start()
    got_slab(2, 0, 0)
    got_slab(2, 0, 1)
    unit(((2, 0),), 0, (0, 1))
    end_group(1, 1)
    have_group(1, 1)
    on_other(got_xi)
    unit(((0, 0), (0, 1), (1, 0), (3, 0), (2, 0)), 1, (1,))
    end_group(1, 0)
    got_slab(3, 1, 1)
    got_slab(1, 1, 0)
    unit(((1, 1), (3, 1)), 0, (0, 1))
    unit(((1, 1), (3, 1)), 1, (1,))
    have_group(1, 0)
    unit(((0, 0), (0, 1), (1, 0), (3, 0), (2, 0), (1, 1), (3, 1)), 1, (0,))
    pl.semaphore_wait(pair_ready, 1)
    send_out(0)
    got_slab(2, 1, 0)
    got_slab(2, 1, 1)
    unit(((2, 1),), 1, (0, 1))
    send_out(1, (1,))
    unit(((2, 1),), 0, (0, 1))
    send_out(1, (0,))

    for b in range(2):
        pltpu.make_async_copy(all_but_one(arrived, b), all_but_one(arrived, b), out_recv.at[b]).wait()
        same = jnp.sum(arrived[b, :owners], axis=0)
        crossed = jnp.sum(arrived[b, owners:], axis=0)
        for r in range(4):
            dy = [d for d, place in ROW_OF_DY.items() if place == b * 2 + r // 2][0]
            eh = r % 2
            k = (flip(zh, eh) * NY + (y + dy) % NY) * 2
            for kk in range(2):
                a = r * 2 + kk
                c = (r ^ 1) * 2 + kk
                o_ref[pl.ds(k + kk, 1), :] = (same[a : a + 1] + crossed[c : c + 1])[:, :own]

    for kk in range(2):
        for eh in range(2):
            y_copy(0, eh, kk, True).wait_send()
            y_copy(0, eh, kk, False).wait_send()
        y_copy(3, kk, 0, True).wait_send()
        y_copy(1, kk, 1, False).wait_send()
        z_copy_t(kk).wait_send()
        z_onward_t(kk).wait_send()
    z_copy_j(1).wait_send()

    @on_source
    def _():
        for hr in range(2):
            z_onward_x(hr).wait_send()
            for el in range(2):
                for dx in (1, 3):
                    x_copy(hr, el, dx).wait_send()
                    x_onward(hr, el, dx).wait_send()
                for dx in range(NX):
                    pair_copy(hr, el, dx).wait_send()

    for b in range(2):
        pltpu.make_async_copy(all_but_one(stage, b), all_but_one(stage, b), out_send.at[b]).wait()


def shards(coeffs, tensor):
    cells, width = coeffs.shape
    outputs, inner, full = tensor.shape
    owners = lax.axis_size("idx")
    return pl.pallas_call(
        kernel,
        out_shape=jax.ShapeDtypeStruct((16, cells // owners), F32),
        in_specs=[pl.BlockSpec(memory_space=pltpu.HBM)] * 2,
        out_specs=pl.BlockSpec(memory_space=pltpu.VMEM),
        scratch_shapes=[
            pltpu.VMEM((cells, width), BF16),
            pltpu.VMEM((2, inner, 2 * NX * width), BF16),
            pltpu.VMEM((2, inner, 2 * NX * width), BF16),
            pltpu.VMEM((16, inner, 2 * NX * width), BF16),
            pltpu.VMEM((2, width, cells), BF16),
            pltpu.VMEM((2, 2 * NX * width, cells), BF16),
            pltpu.VMEM((2, 16, cells), F32),
            pltpu.VMEM((2, 2 * owners, 8, 128), F32),
            pltpu.VMEM((2, 2 * owners, 8, 128), F32),
            pltpu.SemaphoreType.DMA,
            pltpu.SemaphoreType.DMA((4,)),
            pltpu.SemaphoreType.DMA((12,)),
            pltpu.SemaphoreType.DMA((7,)),
            pltpu.SemaphoreType.DMA((16,)),
            pltpu.SemaphoreType.DMA((16,)),
            pltpu.SemaphoreType.DMA((2,)),
            pltpu.SemaphoreType.DMA((16,)),
            pltpu.SemaphoreType.DMA((2,)),
            pltpu.SemaphoreType.DMA,
            pltpu.SemaphoreType.DMA((16,)),
            pltpu.SemaphoreType.DMA((2,)),
            pltpu.SemaphoreType.REGULAR,
            pltpu.SemaphoreType.REGULAR,
        ],
        compiler_params=pltpu.CompilerParams(
            collective_id=0, has_side_effects=True, vmem_limit_bytes=40 * 1024 * 1024
        ),
    )(
        pltpu.with_memory_space_constraint(coeffs, pltpu.HBM),
        pltpu.with_memory_space_constraint(tensor.reshape(outputs * inner, full), pltpu.HBM),
    )


def solution(mesh):
    return jax.shard_map(
        shards,
        mesh=mesh,
        in_specs=(P("cell", "idx"), P("cell", "idx", None)),
        out_specs=P(None, ("cell", "idx")),
        check_vma=False,
    )
```

```python
import jax
import jax.numpy as jnp
from jax import lax
from jax.experimental import pallas as pl
from jax.experimental.pallas import tpu as pltpu
from jax.sharding import PartitionSpec as P

F32 = jnp.float32
BF16 = jnp.bfloat16
NX = 4
NY = 4
ROW_OF_DY = {0: 0, 1: 1, 3: 2, 2: 3}


def flip(bit, other):
    return 1 - bit if other else bit


def kernel(
    x_hbm, t_hbm, o_ref,
    xin, outbox, passing, slab, xi, xj, outp, stage, arrived,
    in_sem, t_sem, y_send, z_send, x_send, pair_send, out_send,
    slab_recv, pass_recv, xi_recv, xj_recv, out_recv, ready, pair_ready,
):
    cell = lax.axis_index("cell")
    idx = lax.axis_index("idx")
    zh = cell // NY
    y = cell % NY
    core = idx % 2
    x = (idx // 2) % NX
    zl = idx // (2 * NX)
    cells, width = x_hbm.shape
    line = NX * width
    owners = lax.axis_size("idx")
    own = cells // owners

    def device(dx=0, dy=0, e=0, other_core=0):
        return {
            "cell": flip(zh, e // 2) * NY + (y + dy) % NY,
            "idx": (flip(zl, e % 2) * NX + (x + dx) % NX) * 2 + flip(core, other_core),
        }

    def copy_to(src, dst, send, recv, dev):
        return pltpu.make_async_remote_copy(
            src_ref=src, dst_ref=dst, send_sem=send, recv_sem=recv,
            device_id=dev, device_id_type=pl.DeviceIdType.MESH,
        )

    def signal(sem, dev):
        pl.semaphore_signal(sem, inc=1, device_id=dev, device_id_type=pl.DeviceIdType.MESH)

    barrier = pltpu.get_barrier_semaphore()
    peers = [device(dy=1), device(dy=3), device(other_core=1)]
    peers += [device(dx=dx) for dx in (1, 2, 3)] + [device(e=e) for e in (1, 2, 3)]
    for peer in peers:
        signal(barrier, peer)

    x_in = pltpu.make_async_copy(x_hbm, xin, in_sem)
    x_in.start()

    def part_of(eh, kk):
        return outbox.at[kk] if eh else slab.at[kk]

    for eh in range(2):
        for kk in range(2):
            for el in range(2):
                for dx in range(NX):
                    block = (flip(zl, el) * NX + (x + dx) % NX) * 2 + flip(zh, eh)
                    pltpu.make_async_copy(
                        t_hbm.at[pl.ds(kk * width, width), pl.ds(pl.multiple_of(block * width, width), width)],
                        part_of(eh, kk).at[:, pl.ds(el * line + dx * width, width)],
                        t_sem.at[eh * 2 + kk],
                    ).start()

    x_in.wait()
    for t in range(cells // width):
        xi[0, :, t * width : (t + 1) * width] = jnp.transpose(
            xin[t * width : (t + 1) * width, :]
        )

    source = core == zh

    def on_source(f):
        pl.when(source)(f)

    def on_other(f):
        pl.when(jnp.logical_not(source))(f)

    @on_source
    def _():
        xj[0, :width, :] = xi[0]

    for eh in range(2):
        for kk in range(2):
            pltpu.make_async_copy(part_of(eh, kk), part_of(eh, kk), t_sem.at[eh * 2 + kk]).wait()

    pl.semaphore_wait(barrier, len(peers))

    for dx in (1, 2, 3):
        signal(ready, device(dx=dx))

    def slot(dy, eh, kk):
        return dy * 4 + eh * 2 + kk

    def y_copy(dy, eh, kk, up):
        n = (0 if up else 6) + (eh * 2 + kk if dy == 0 else 4 + eh)
        there = slot((dy - (1 if up else -1)) % NY, eh, kk)
        return copy_to(
            slab.at[slot(dy, eh, kk)], slab.at[there],
            y_send.at[n], slab_recv.at[there], device(dy=1 if up else 3),
        )

    def block_of(hr, el, dx):
        return xj.at[hr, pl.ds(el * line + dx * width, width)]

    def half_of(hr, el, part):
        return xj.at[hr, pl.ds(el * line + 2 * width + part * (width // 2), width // 2)]

    def number(hr, el, dx):
        return (hr * 2 + el) * NX + dx

    def z_copy_t(kk):
        return copy_to(outbox.at[kk], passing.at[kk], z_send.at[kk], pass_recv.at[kk], device(e=3 if kk else 1))

    def z_onward_t(kk):
        there = slot(0, 1, kk)
        return copy_to(
            passing.at[kk], slab.at[there], z_send.at[2 + kk], slab_recv.at[there], device(e=1 if kk else 3)
        )

    def z_onward_x(hr):
        return copy_to(block_of(hr, 1, 0), xi.at[1], z_send.at[5 + hr], xi_recv, device(e=1 if hr else 3))

    def z_copy_j(e):
        hr = e // 2
        return copy_to(
            xi.at[0], block_of(hr, 1, 0), z_send.at[4], xj_recv.at[number(hr, 1, 0)], device(e=e)
        )

    def first_of(hr, el):
        return block_of(hr, el, 0) if el else xi.at[hr]

    def x_copy(hr, el, dx):
        n = number(hr, el, {1: 0, 3: 1, 2: 2}[dx])
        there = NX - dx
        return copy_to(
            first_of(hr, el), block_of(hr, el, there),
            x_send.at[n], xj_recv.at[number(hr, el, there)], device(dx=dx),
        )

    def x_onward(hr, el, dx):
        part = 0 if dx == 1 else 1
        src = xj.at[hr, pl.ds(el * line + dx * width + part * (width // 2), width // 2)]
        return copy_to(
            src, half_of(hr, el, part), x_send.at[number(hr, el, 2 + part)],
            xj_recv.at[number(hr, el, 2)], device(dx=NX - dx),
        )

    def pair_copy(hr, el, dx):
        src = first_of(hr, el) if dx == 0 else block_of(hr, el, dx)
        n = number(hr, el, dx)
        return copy_to(
            src, block_of(hr, el, dx), pair_send.at[n], xj_recv.at[n], device(other_core=1)
        )

    def got_slab(dy, eh, kk):
        there = slab.at[slot(dy, eh, kk)]
        pltpu.make_async_copy(there, there, slab_recv.at[slot(dy, eh, kk)]).wait()

    def got_passing(kk):
        pltpu.make_async_copy(passing.at[kk], passing.at[kk], pass_recv.at[kk]).wait()

    def got_xi():
        pltpu.make_async_copy(xi.at[1], xi.at[1], xi_recv).wait()

    def got_xj(hr, el, dx):
        there = block_of(hr, el, dx)
        pltpu.make_async_copy(there, there, xj_recv.at[number(hr, el, dx)]).wait()

    def y_own(eh, kk):
        y_copy(0, eh, kk, True).start()
        y_copy(0, eh, 1 - kk, False).start()

    def spread(hr, el):
        x_copy(hr, el, 1).start()
        x_copy(hr, el, 3).start()
        pair_copy(hr, el, 0).start()

    def start_group(hr, el):
        @on_source
        def _():
            if el:
                got_xj(hr, el, 0)
            elif hr:
                got_xi()
            spread(hr, el)
            if hr and not el:
                xj[1, :width, :] = xi[1]

    def pass_on(hr, el):
        @on_source
        def _():
            for dx in (1, 3):
                got_xj(hr, el, dx)
                x_onward(hr, el, dx).start()

    def pair_on(hr, el):
        @on_source
        def _():
            for dx in (1, 3):
                pair_copy(hr, el, dx).start()

    def end_group(hr, el):
        @on_source
        def _():
            got_xj(hr, el, 2)
            pair_copy(hr, el, 2).start()

    def have_group(hr, el):
        @on_other
        def _():
            for dx in range(NX):
                got_xj(hr, el, dx)

    begun = set()

    def unit(pieces, hr, els):
        deep = pl.ds(els[0] * line, len(els) * line)

        def tile(n, _):
            cols = pl.ds(pl.multiple_of(n * 256, 256), 256)
            w = xj[hr, deep, cols]
            rows = xi[hr, :, cols].astype(F32)
            for dy, eh in pieces:
                at = slot(dy, eh, 0)
                left = slab[at : at + 2, :, deep].reshape(2 * width, len(els) * line)
                mixed = jnp.dot(left, w, preferred_element_type=F32)
                terms = mixed.reshape(2, width, 256) * rows[None]
                part = jnp.sum(terms.reshape(2, width // 8, 8, 256), axis=1)
                out = jnp.sum(part, axis=1)
                row = ROW_OF_DY[dy] * 4 + eh * 2
                if (dy, eh, hr) in begun:
                    out = out + outp[hr, row : row + 2, cols]
                outp[hr, row : row + 2, cols] = out
            return 0

        lax.fori_loop(0, cells // 256, tile, 0, unroll=True)
        begun.update((dy, eh, hr) for dy, eh in pieces)

    def send_out(b, hrs=(1, 0)):
        for hr in hrs:
            rows = outp[hr, b * 8 : b * 8 + 8, :]
            for q in range(owners):
                first = q * own // 128 * 128
                shift = q * own - first
                window = rows[:, first : first + 256] if first + 256 <= cells else rows[:, first : first + 128]
                if shift:
                    window = pltpu.roll(window, window.shape[1] - shift, 1)
                stage[b, hr * owners + q] = window[:, :128]

            for j in range(1 - hr, owners):
                q = (idx + j) % owners
                copy_to(
                    stage.at[b, hr * owners + q], arrived.at[b, hr * owners + idx],
                    out_send.at[b], out_recv.at[b],
                    {"cell": flip(zh, hr) * NY + y, "idx": q},
                ).start()

        if 0 in hrs:
            arrived[b, idx] = stage[b, idx]

    def all_but_one(ref, b):
        return ref.at[b, pl.ds(0, 2 * owners - 1)]

    y_own(0, 0)
    y_own(0, 1)

    @on_source
    def _():
        z_copy_j(1).start()
        spread(0, 0)

    z_copy_t(0).start()
    z_copy_t(1).start()
    on_other(z_copy_j(3).start)

    pass_on(0, 0)
    pair_on(0, 0)
    got_slab(3, 0, 0)
    got_slab(1, 0, 1)
    y_copy(3, 0, 0, True).start()
    y_copy(1, 0, 1, False).start()
    start_group(0, 1)
    end_group(0, 0)
    start_group(1, 1)
    on_source(z_onward_x(1).start)
    for kk in range(2):
        got_passing(kk)
        z_onward_t(kk).start()
    on_source(z_onward_x(0).start)

    pass_on(0, 1)
    pair_on(0, 1)
    have_group(0, 0)
    got_slab(3, 0, 1)
    got_slab(1, 0, 0)
    unit(((0, 0), (1, 0), (3, 0)), 0, (0,))
    got_slab(0, 1, 0)
    y_copy(0, 1, 0, True).start()
    start_group(1, 0)
    pass_on(1, 1)
    got_slab(0, 1, 1)
    y_copy(0, 1, 1, False).start()
    y_copy(0, 1, 1, True).start()
    y_copy(0, 1, 0, False).start()
    end_group(0, 1)
    pair_on(1, 1)
    pl.semaphore_wait(ready, 3)
    signal(pair_ready, device(other_core=1))
    unit(((0, 1),), 0, (0,))
    have_group(0, 1)
    unit(((0, 0), (1, 0), (3, 0), (0, 1)), 0, (1,))
    got_slab(3, 1, 0)
    y_copy(3, 1, 0, True).start()
    pass_on(1, 0)
    got_slab(1, 1, 1)
    y_copy(1, 1, 1, False).start()
    got_slab(2, 0, 0)
    got_slab(2, 0, 1)
    unit(((2, 0),), 0, (0, 1))
    end_group(1, 1)
    pair_on(1, 0)
    have_group(1, 1)
    on_other(got_xi)
    unit(((0, 0), (0, 1), (1, 0), (3, 0), (2, 0)), 1, (1,))
    end_group(1, 0)
    got_slab(3, 1, 1)
    got_slab(1, 1, 0)
    unit(((1, 1), (3, 1)), 0, (0, 1))
    unit(((1, 1), (3, 1)), 1, (1,))
    have_group(1, 0)
    unit(((0, 0), (0, 1), (1, 0), (3, 0), (2, 0), (1, 1), (3, 1)), 1, (0,))
    pl.semaphore_wait(pair_ready, 1)
    send_out(0)
    got_slab(2, 1, 0)
    got_slab(2, 1, 1)
    unit(((2, 1),), 1, (0, 1))
    send_out(1, (1,))
    unit(((2, 1),), 0, (0, 1))
    send_out(1, (0,))

    for kk in range(2):
        for eh in range(2):
            y_copy(0, eh, kk, True).wait_send()
            y_copy(0, eh, kk, False).wait_send()
        y_copy(3, kk, 0, True).wait_send()
        y_copy(1, kk, 1, False).wait_send()
        z_copy_t(kk).wait_send()
        z_onward_t(kk).wait_send()
    z_copy_j(1).wait_send()

    @on_source
    def _():
        for hr in range(2):
            z_onward_x(hr).wait_send()
            for el in range(2):
                for dx in (1, 3):
                    x_copy(hr, el, dx).wait_send()
                    x_onward(hr, el, dx).wait_send()
                for dx in range(NX):
                    pair_copy(hr, el, dx).wait_send()

    for b in range(2):
        pltpu.make_async_copy(all_but_one(stage, b), all_but_one(stage, b), out_send.at[b]).wait()

    for b in range(2):
        pltpu.make_async_copy(all_but_one(arrived, b), all_but_one(arrived, b), out_recv.at[b]).wait()
        same = jnp.sum(arrived[b, :owners], axis=0)
        crossed = jnp.sum(arrived[b, owners:], axis=0)
        for r in range(4):
            dy = [d for d, place in ROW_OF_DY.items() if place == b * 2 + r // 2][0]
            eh = r % 2
            k = (flip(zh, eh) * NY + (y + dy) % NY) * 2
            for kk in range(2):
                a = r * 2 + kk
                c = (r ^ 1) * 2 + kk
                o_ref[pl.ds(k + kk, 1), :] = (same[a : a + 1] + crossed[c : c + 1])[:, :own]


def shards(coeffs, tensor):
    cells, width = coeffs.shape
    outputs, inner, full = tensor.shape
    owners = lax.axis_size("idx")
    return pl.pallas_call(
        kernel,
        out_shape=jax.ShapeDtypeStruct((16, cells // owners), F32),
        in_specs=[pl.BlockSpec(memory_space=pltpu.HBM)] * 2,
        out_specs=pl.BlockSpec(memory_space=pltpu.VMEM),
        scratch_shapes=[
            pltpu.VMEM((cells, width), BF16),
            pltpu.VMEM((2, inner, 2 * NX * width), BF16),
            pltpu.VMEM((2, inner, 2 * NX * width), BF16),
            pltpu.VMEM((16, inner, 2 * NX * width), BF16),
            pltpu.VMEM((2, width, cells), BF16),
            pltpu.VMEM((2, 2 * NX * width, cells), BF16),
            pltpu.VMEM((2, 16, cells), F32),
            pltpu.VMEM((2, 2 * owners, 8, 128), F32),
            pltpu.VMEM((2, 2 * owners, 8, 128), F32),
            pltpu.SemaphoreType.DMA,
            pltpu.SemaphoreType.DMA((4,)),
            pltpu.SemaphoreType.DMA((12,)),
            pltpu.SemaphoreType.DMA((7,)),
            pltpu.SemaphoreType.DMA((16,)),
            pltpu.SemaphoreType.DMA((16,)),
            pltpu.SemaphoreType.DMA((2,)),
            pltpu.SemaphoreType.DMA((16,)),
            pltpu.SemaphoreType.DMA((2,)),
            pltpu.SemaphoreType.DMA,
            pltpu.SemaphoreType.DMA((16,)),
            pltpu.SemaphoreType.DMA((2,)),
            pltpu.SemaphoreType.REGULAR,
            pltpu.SemaphoreType.REGULAR,
        ],
        compiler_params=pltpu.CompilerParams(
            collective_id=0, has_side_effects=True, vmem_limit_bytes=40 * 1024 * 1024
        ),
    )(
        pltpu.with_memory_space_constraint(coeffs, pltpu.HBM),
        pltpu.with_memory_space_constraint(tensor.reshape(outputs * inner, full), pltpu.HBM),
    )


def solution(mesh):
    return jax.shard_map(
        shards,
        mesh=mesh,
        in_specs=(P("cell", "idx"), P("cell", "idx", None)),
        out_specs=P(None, ("cell", "idx")),
        check_vma=False,
    )
```

```python
import jax
import jax.numpy as jnp
from jax import lax
from jax.experimental import pallas as pl
from jax.experimental.pallas import tpu as pltpu
from jax.sharding import PartitionSpec as P

F32 = jnp.float32
BF16 = jnp.bfloat16
NX = 4
NY = 4
ROW_OF_DY = {0: 0, 1: 1, 3: 2, 2: 3}


def flip(bit, other):
    return 1 - bit if other else bit


def kernel(
    x_hbm, t_hbm, o_ref,
    xin, outbox, passing, slab, xi, xj, outp, stage, arrived,
    in_sem, t_sem, y_send, z_send, x_send, pair_send, out_send,
    slab_recv, pass_recv, xi_recv, xj_recv, out_recv, ready, pair_ready, half_send, half_recv,
):
    cell = lax.axis_index("cell")
    idx = lax.axis_index("idx")
    zh = cell // NY
    y = cell % NY
    core = idx % 2
    x = (idx // 2) % NX
    zl = idx // (2 * NX)
    cells, width = x_hbm.shape
    line = NX * width
    owners = lax.axis_size("idx")
    own = cells // owners

    def device(dx=0, dy=0, e=0, other_core=0):
        return {
            "cell": flip(zh, e // 2) * NY + (y + dy) % NY,
            "idx": (flip(zl, e % 2) * NX + (x + dx) % NX) * 2 + flip(core, other_core),
        }

    def copy_to(src, dst, send, recv, dev):
        return pltpu.make_async_remote_copy(
            src_ref=src, dst_ref=dst, send_sem=send, recv_sem=recv,
            device_id=dev, device_id_type=pl.DeviceIdType.MESH,
        )

    def signal(sem, dev):
        pl.semaphore_signal(sem, inc=1, device_id=dev, device_id_type=pl.DeviceIdType.MESH)

    barrier = pltpu.get_barrier_semaphore()
    peers = [device(dy=1), device(dy=3), device(other_core=1)]
    peers += [device(dx=dx) for dx in (1, 2, 3)] + [device(e=e) for e in (1, 2, 3)]
    for peer in peers:
        signal(barrier, peer)

    x_in = pltpu.make_async_copy(x_hbm, xin, in_sem)
    x_in.start()

    def part_of(eh, kk):
        return outbox.at[kk] if eh else slab.at[kk]

    for eh in range(2):
        for kk in range(2):
            for el in range(2):
                for dx in range(NX):
                    block = (flip(zl, el) * NX + (x + dx) % NX) * 2 + flip(zh, eh)
                    pltpu.make_async_copy(
                        t_hbm.at[pl.ds(kk * width, width), pl.ds(pl.multiple_of(block * width, width), width)],
                        part_of(eh, kk).at[:, pl.ds(el * line + dx * width, width)],
                        t_sem.at[eh * 2 + kk],
                    ).start()

    x_in.wait()
    for t in range(cells // width):
        xi[0, :, t * width : (t + 1) * width] = jnp.transpose(
            xin[t * width : (t + 1) * width, :]
        )

    source = core == zh

    def on_source(f):
        pl.when(source)(f)

    def on_other(f):
        pl.when(jnp.logical_not(source))(f)

    @on_source
    def _():
        xj[0, :width, :] = xi[0]

    for eh in range(2):
        for kk in range(2):
            pltpu.make_async_copy(part_of(eh, kk), part_of(eh, kk), t_sem.at[eh * 2 + kk]).wait()

    pl.semaphore_wait(barrier, len(peers))

    for dx in (1, 2, 3):
        signal(ready, device(dx=dx))

    def slot(dy, eh, kk):
        return dy * 4 + eh * 2 + kk

    def y_copy(dy, eh, kk, up):
        n = (0 if up else 6) + (eh * 2 + kk if dy == 0 else 4 + eh)
        there = slot((dy - (1 if up else -1)) % NY, eh, kk)
        return copy_to(
            slab.at[slot(dy, eh, kk)], slab.at[there],
            y_send.at[n], slab_recv.at[there], device(dy=1 if up else 3),
        )

    def block_of(hr, el, dx):
        return xj.at[hr, pl.ds(el * line + dx * width, width)]

    def half_of(hr, el, part):
        return xj.at[hr, pl.ds(el * line + 2 * width + part * (width // 2), width // 2)]

    def number(hr, el, dx):
        return (hr * 2 + el) * NX + dx

    def z_copy_t(kk):
        return copy_to(outbox.at[kk], passing.at[kk], z_send.at[kk], pass_recv.at[kk], device(e=3 if kk else 1))

    def z_onward_t(kk):
        there = slot(0, 1, kk)
        return copy_to(
            passing.at[kk], slab.at[there], z_send.at[2 + kk], slab_recv.at[there], device(e=1 if kk else 3)
        )

    def z_onward_x(hr):
        return copy_to(block_of(hr, 1, 0), xi.at[1], z_send.at[5 + hr], xi_recv, device(e=1 if hr else 3))

    def z_copy_j(e):
        hr = e // 2
        return copy_to(
            xi.at[0], block_of(hr, 1, 0), z_send.at[4], xj_recv.at[number(hr, 1, 0)], device(e=e)
        )

    def first_of(hr, el):
        return block_of(hr, el, 0) if el else xi.at[hr]

    def x_copy(hr, el, dx):
        n = number(hr, el, {1: 0, 3: 1, 2: 2}[dx])
        there = NX - dx
        return copy_to(
            first_of(hr, el), block_of(hr, el, there),
            x_send.at[n], xj_recv.at[number(hr, el, there)], device(dx=dx),
        )

    def x_onward(hr, el, dx):
        part = 0 if dx == 1 else 1
        src = xj.at[hr, pl.ds(el * line + dx * width + part * (width // 2), width // 2)]
        return copy_to(
            src, half_of(hr, el, part), x_send.at[number(hr, el, 2 + part)],
            half_recv.at[(hr * 2 + el) * 2 + part], device(dx=NX - dx),
        )

    def pair_copy(hr, el, dx):
        src = first_of(hr, el) if dx == 0 else block_of(hr, el, dx)
        n = number(hr, el, dx)
        return copy_to(
            src, block_of(hr, el, dx), pair_send.at[n], xj_recv.at[n], device(other_core=1)
        )

    def pair_half(hr, el, part):
        n = (hr * 2 + el) * 2 + part
        there = half_of(hr, el, part)
        return copy_to(there, there, half_send.at[n], half_recv.at[n], device(other_core=1))

    def got_half(hr, el, part):
        there = half_of(hr, el, part)
        pltpu.make_async_copy(there, there, half_recv.at[(hr * 2 + el) * 2 + part]).wait()

    def got_slab(dy, eh, kk):
        there = slab.at[slot(dy, eh, kk)]
        pltpu.make_async_copy(there, there, slab_recv.at[slot(dy, eh, kk)]).wait()

    def got_passing(kk):
        pltpu.make_async_copy(passing.at[kk], passing.at[kk], pass_recv.at[kk]).wait()

    def got_xi():
        pltpu.make_async_copy(xi.at[1], xi.at[1], xi_recv).wait()

    def got_xj(hr, el, dx):
        there = block_of(hr, el, dx)
        pltpu.make_async_copy(there, there, xj_recv.at[number(hr, el, dx)]).wait()

    def y_own(eh, kk):
        y_copy(0, eh, kk, True).start()
        y_copy(0, eh, 1 - kk, False).start()

    def spread(hr, el):
        x_copy(hr, el, 1).start()
        x_copy(hr, el, 3).start()
        pair_copy(hr, el, 0).start()

    def start_group(hr, el):
        @on_source
        def _():
            if el:
                got_xj(hr, el, 0)
            elif hr:
                got_xi()
            spread(hr, el)
            if hr and not el:
                xj[1, :width, :] = xi[1]

    def pass_on(hr, el):
        @on_source
        def _():
            for dx in (1, 3):
                got_xj(hr, el, dx)
                x_onward(hr, el, dx).start()

    def pair_on(hr, el):
        @on_source
        def _():
            for dx in (1, 3):
                pair_copy(hr, el, dx).start()

    def end_group(hr, el):
        @on_source
        def _():
            for part in range(2):
                got_half(hr, el, part)
                pair_half(hr, el, part).start()

    def have_group(hr, el):
        @on_other
        def _():
            for dx in (0, 1, 3):
                got_xj(hr, el, dx)
            for part in range(2):
                got_half(hr, el, part)

    begun = set()

    def unit(pieces, hr, els):
        deep = pl.ds(els[0] * line, len(els) * line)

        def tile(n, _):
            cols = pl.ds(pl.multiple_of(n * 256, 256), 256)
            w = xj[hr, deep, cols]
            rows = xi[hr, :, cols].astype(F32)
            for dy, eh in pieces:
                at = slot(dy, eh, 0)
                left = slab[at : at + 2, :, deep].reshape(2 * width, len(els) * line)
                mixed = jnp.dot(left, w, preferred_element_type=F32)
                terms = mixed.reshape(2, width, 256) * rows[None]
                part = jnp.sum(terms.reshape(2, width // 8, 8, 256), axis=1)
                out = jnp.sum(part, axis=1)
                row = ROW_OF_DY[dy] * 4 + eh * 2
                if (dy, eh, hr) in begun:
                    out = out + outp[hr, row : row + 2, cols]
                outp[hr, row : row + 2, cols] = out
            return 0

        lax.fori_loop(0, cells // 256, tile, 0, unroll=True)
        begun.update((dy, eh, hr) for dy, eh in pieces)

    def send_out(b, hrs=(1, 0)):
        for hr in hrs:
            rows = outp[hr, b * 8 : b * 8 + 8, :]
            for q in range(owners):
                first = q * own // 128 * 128
                shift = q * own - first
                window = rows[:, first : first + 256] if first + 256 <= cells else rows[:, first : first + 128]
                if shift:
                    window = pltpu.roll(window, window.shape[1] - shift, 1)
                stage[b, hr * owners + q] = window[:, :128]

            for j in range(1 - hr, owners):
                q = (idx + j) % owners
                copy_to(
                    stage.at[b, hr * owners + q], arrived.at[b, hr * owners + idx],
                    out_send.at[b], out_recv.at[b],
                    {"cell": flip(zh, hr) * NY + y, "idx": q},
                ).start()

        if 0 in hrs:
            arrived[b, idx] = stage[b, idx]

    def all_but_one(ref, b):
        return ref.at[b, pl.ds(0, 2 * owners - 1)]

    y_own(0, 0)
    y_own(0, 1)

    @on_source
    def _():
        z_copy_j(1).start()
        spread(0, 0)

    z_copy_t(0).start()
    z_copy_t(1).start()
    on_other(z_copy_j(3).start)

    pass_on(0, 0)
    pair_on(0, 0)
    got_slab(3, 0, 0)
    got_slab(1, 0, 1)
    y_copy(3, 0, 0, True).start()
    y_copy(1, 0, 1, False).start()
    start_group(0, 1)
    end_group(0, 0)
    start_group(1, 1)
    on_source(z_onward_x(1).start)
    for kk in range(2):
        got_passing(kk)
        z_onward_t(kk).start()
    on_source(z_onward_x(0).start)

    pass_on(0, 1)
    pair_on(0, 1)
    have_group(0, 0)
    got_slab(3, 0, 1)
    got_slab(1, 0, 0)
    unit(((0, 0), (1, 0), (3, 0)), 0, (0,))
    got_slab(0, 1, 0)
    y_copy(0, 1, 0, True).start()
    start_group(1, 0)
    pass_on(1, 1)
    got_slab(0, 1, 1)
    y_copy(0, 1, 1, False).start()
    y_copy(0, 1, 1, True).start()
    y_copy(0, 1, 0, False).start()
    end_group(0, 1)
    pair_on(1, 1)
    pl.semaphore_wait(ready, 3)
    signal(pair_ready, device(other_core=1))
    unit(((0, 1),), 0, (0,))
    have_group(0, 1)
    unit(((0, 0), (1, 0), (3, 0), (0, 1)), 0, (1,))
    got_slab(3, 1, 0)
    y_copy(3, 1, 0, True).start()
    pass_on(1, 0)
    got_slab(1, 1, 1)
    y_copy(1, 1, 1, False).start()
    got_slab(2, 0, 0)
    got_slab(2, 0, 1)
    unit(((2, 0),), 0, (0, 1))
    end_group(1, 1)
    pair_on(1, 0)
    have_group(1, 1)
    on_other(got_xi)
    unit(((0, 0), (0, 1), (1, 0), (3, 0), (2, 0)), 1, (1,))
    end_group(1, 0)
    got_slab(3, 1, 1)
    got_slab(1, 1, 0)
    unit(((1, 1), (3, 1)), 0, (0, 1))
    unit(((1, 1), (3, 1)), 1, (1,))
    have_group(1, 0)
    unit(((0, 0), (0, 1), (1, 0), (3, 0), (2, 0), (1, 1), (3, 1)), 1, (0,))
    pl.semaphore_wait(pair_ready, 1)
    send_out(0)
    got_slab(2, 1, 0)
    got_slab(2, 1, 1)
    unit(((2, 1),), 1, (0, 1))
    send_out(1, (1,))
    unit(((2, 1),), 0, (0, 1))
    send_out(1, (0,))

    for kk in range(2):
        for eh in range(2):
            y_copy(0, eh, kk, True).wait_send()
            y_copy(0, eh, kk, False).wait_send()
        y_copy(3, kk, 0, True).wait_send()
        y_copy(1, kk, 1, False).wait_send()
        z_copy_t(kk).wait_send()
        z_onward_t(kk).wait_send()
    z_copy_j(1).wait_send()

    @on_source
    def _():
        for hr in range(2):
            z_onward_x(hr).wait_send()
            for el in range(2):
                for dx in (1, 3):
                    x_copy(hr, el, dx).wait_send()
                    x_onward(hr, el, dx).wait_send()
                for dx in (0, 1, 3):
                    pair_copy(hr, el, dx).wait_send()
                for part in range(2):
                    pair_half(hr, el, part).wait_send()

    for b in range(2):
        pltpu.make_async_copy(all_but_one(stage, b), all_but_one(stage, b), out_send.at[b]).wait()

    for b in range(2):
        pltpu.make_async_copy(all_but_one(arrived, b), all_but_one(arrived, b), out_recv.at[b]).wait()
        same = jnp.sum(arrived[b, :owners], axis=0)
        crossed = jnp.sum(arrived[b, owners:], axis=0)
        for r in range(4):
            dy = [d for d, place in ROW_OF_DY.items() if place == b * 2 + r // 2][0]
            eh = r % 2
            k = (flip(zh, eh) * NY + (y + dy) % NY) * 2
            for kk in range(2):
                a = r * 2 + kk
                c = (r ^ 1) * 2 + kk
                o_ref[pl.ds(k + kk, 1), :] = (same[a : a + 1] + crossed[c : c + 1])[:, :own]


def shards(coeffs, tensor):
    cells, width = coeffs.shape
    outputs, inner, full = tensor.shape
    owners = lax.axis_size("idx")
    return pl.pallas_call(
        kernel,
        out_shape=jax.ShapeDtypeStruct((16, cells // owners), F32),
        in_specs=[pl.BlockSpec(memory_space=pltpu.HBM)] * 2,
        out_specs=pl.BlockSpec(memory_space=pltpu.VMEM),
        scratch_shapes=[
            pltpu.VMEM((cells, width), BF16),
            pltpu.VMEM((2, inner, 2 * NX * width), BF16),
            pltpu.VMEM((2, inner, 2 * NX * width), BF16),
            pltpu.VMEM((16, inner, 2 * NX * width), BF16),
            pltpu.VMEM((2, width, cells), BF16),
            pltpu.VMEM((2, 2 * NX * width, cells), BF16),
            pltpu.VMEM((2, 16, cells), F32),
            pltpu.VMEM((2, 2 * owners, 8, 128), F32),
            pltpu.VMEM((2, 2 * owners, 8, 128), F32),
            pltpu.SemaphoreType.DMA,
            pltpu.SemaphoreType.DMA((4,)),
            pltpu.SemaphoreType.DMA((12,)),
            pltpu.SemaphoreType.DMA((7,)),
            pltpu.SemaphoreType.DMA((16,)),
            pltpu.SemaphoreType.DMA((16,)),
            pltpu.SemaphoreType.DMA((2,)),
            pltpu.SemaphoreType.DMA((16,)),
            pltpu.SemaphoreType.DMA((2,)),
            pltpu.SemaphoreType.DMA,
            pltpu.SemaphoreType.DMA((16,)),
            pltpu.SemaphoreType.DMA((2,)),
            pltpu.SemaphoreType.REGULAR,
            pltpu.SemaphoreType.REGULAR,
            pltpu.SemaphoreType.DMA((8,)),
            pltpu.SemaphoreType.DMA((8,)),
        ],
        compiler_params=pltpu.CompilerParams(
            collective_id=0, has_side_effects=True, vmem_limit_bytes=40 * 1024 * 1024
        ),
    )(
        pltpu.with_memory_space_constraint(coeffs, pltpu.HBM),
        pltpu.with_memory_space_constraint(tensor.reshape(outputs * inner, full), pltpu.HBM),
    )


def solution(mesh):
    return jax.shard_map(
        shards,
        mesh=mesh,
        in_specs=(P("cell", "idx"), P("cell", "idx", None)),
        out_specs=P(None, ("cell", "idx")),
        check_vma=False,
    )
```
